256 devices in a mesh: gx: 4 (over x), gy: 4 (over y_lo, core), zt: 16 (over y_hi, z).
Axes of the slice: x: 4, y: 4 (y_hi: 2, y_lo: 2; y = y_hi * 2 + y_lo), z: 8, core: 2. Of those that a mesh axis runs over, the one named last changes fastest.
Arguments:
- gauge_links: float32 [4, 2, 3, 3, 8, 32, 2048], P(None, None, None, None, 'gx', 'gy', 'zt'), may hold values from -1 to 1, as said below
- momenta: float32 [4, 2, 3, 3, 8, 32, 2048], P(None, None, None, None, 'gx', 'gy', 'zt'), may hold values from -4 to 4, as said below
Outputs:
- new_links: float32 [4, 2, 3, 3, 8, 32, 2048], P(None, None, None, None, 'gx', 'gy', 'zt')
- new_momenta: float32 [4, 2, 3, 3, 8, 32, 2048], P(None, None, None, None, 'gx', 'gy', 'zt')
- plaquette: float32 [], replicated
The draws below stay inside these ranges and needn't reach their ends.
Inputs may be any that keep to these rules, and one draw needn't show every extreme that they name: `gauge_links`: every link is a unitary 3 x 3 complex matrix. `momenta`: every momentum is an antihermitian traceless 3 x 3 complex matrix.
All inputs are finite; a program needn't handle non-finite values.
Results may differ from the reference program's by a relative error of at most 0.0001.
Values sent between devices are 32-bit elements; how exact they have to be, the bound alone decides.
No kernel may reach another device: no remote copies, remote signals or barrier semaphores. Data moves between devices by JAX's collectives and lax.ppermute only.
A program may use at most 128 MiB of HBM per device.

```python
import jax
import jax.numpy as jnp

LT = 64
NX = 8
NY = 32
NZ = 32


def times_pair(first, second):
    return (first[0] * second[0] - first[1] * second[1], first[0] * second[1] + first[1] * second[0])


def unitary_from(real_gen, imag_gen):
    identity = jnp.eye(3, dtype=jnp.float32)[:, :, None, None, None, None]
    top_real = identity + 0.5 * real_gen
    top_imag = 0.5 * imag_gen
    low_real = identity - 0.5 * real_gen
    low_imag = -0.5 * imag_gen

    def element(row_index, column):
        return (low_real[row_index % 3, column % 3], low_imag[row_index % 3, column % 3])
    cofactor = []
    for row_index in range(3):
        line = []
        for column in range(3):
            first = times_pair(element(column + 1, row_index + 1), element(column + 2, row_index + 2))
            second = times_pair(element(column + 1, row_index + 2), element(column + 2, row_index + 1))
            line.append((first[0] - second[0], first[1] - second[1]))
        cofactor.append(line)
    determinant = times_pair(element(0, 0), cofactor[0][0])
    for middle in (1, 2):
        extra = times_pair(element(0, middle), cofactor[middle][0])
        determinant = (determinant[0] + extra[0], determinant[1] + extra[1])
    norm_square = determinant[0] * determinant[0] + determinant[1] * determinant[1]
    inverse_det = (determinant[0] / norm_square, -determinant[1] / norm_square)
    real_rows = []
    imag_rows = []
    for row_index in range(3):
        real_line = []
        imag_line = []
        for column in range(3):
            total_real = 0.0
            total_imag = 0.0
            for inner in range(3):
                entry = times_pair(cofactor[inner][column], inverse_det)
                value = times_pair((top_real[row_index, inner], top_imag[row_index, inner]), entry)
                total_real = total_real + value[0]
                total_imag = total_imag + value[1]
            real_line.append(total_real)
            imag_line.append(total_imag)
        real_rows.append(jnp.stack(real_line))
        imag_rows.append(jnp.stack(imag_line))
    return (jnp.stack(real_rows), jnp.stack(imag_rows))


def draw_gauge_links(key, part):
    key_x = jax.random.fold_in(key, 11)
    key_z = jax.random.fold_in(key, 12)
    key_noise = jax.random.fold_in(key, 13)
    order_x = jax.random.uniform(key_x, (NX,), jnp.float32)
    order_z = jax.random.uniform(key_z, (NZ,), jnp.float32)
    strength = 0.4 + 3.0 * order_x[:, None, None, None] * order_z[None, None, :, None]
    strength = jnp.broadcast_to(strength, (NX, NY, NZ, LT)).reshape(NX, NY, NZ * LT)
    shape = (2, 3, 3, 4, NX, NY, NZ * LT)
    noise = jax.random.normal(key_noise, shape, jnp.float32)
    identity = jnp.eye(3, dtype=jnp.float32)[:, :, None, None, None, None]
    real_gen = 0.5 * (noise[0] - jnp.swapaxes(noise[0], 0, 1)) * strength
    imag_sym = 0.5 * (noise[1] + jnp.swapaxes(noise[1], 0, 1))
    trace_imag = (imag_sym[0, 0] + imag_sym[1, 1] + imag_sym[2, 2]) / 3.0
    imag_gen = (imag_sym - trace_imag * identity) * strength
    real_link, imag_link = unitary_from(real_gen, imag_gen)
    result = jnp.stack([real_link, imag_link])
    result = jnp.moveaxis(result, 3, 0)
    return jnp.clip(result, -1.0, 1.0).astype(jnp.float32)


def draw_momenta(key, part):
    key_base = jax.random.fold_in(key, 21)
    shape = (4, 2, 3, 3, NX, NY, NZ * LT)
    base = jax.random.truncated_normal(key_base, -3.0, 3.0, shape, jnp.float32)
    identity = jnp.eye(3, dtype=jnp.float32)[:, :, None, None, None]
    real_part = 0.5 * (base[:, 0] - jnp.swapaxes(base[:, 0], 1, 2))
    imag_part = 0.5 * (base[:, 1] + jnp.swapaxes(base[:, 1], 1, 2))
    trace_imag = (imag_part[:, 0, 0] + imag_part[:, 1, 1] + imag_part[:, 2, 2]) / 3.0
    imag_part = imag_part - trace_imag[:, None, None] * identity
    return jnp.stack([real_part, imag_part], axis=1).astype(jnp.float32)


def setup_inputs(seed: int = 0) -> dict:
    keys = jax.random.split(jax.random.key(seed), 3)
    gauge_links = draw_gauge_links(jax.random.fold_in(keys[2], 71), 0)
    momenta = draw_momenta(jax.random.fold_in(keys[2], 71), 0)
    return dict(gauge_links=gauge_links, momenta=momenta)


kick_size = 0.25
step_size = 0.2


def matrix_product(left, right):
    real_part = 0.0
    imag_part = 0.0
    for inner in range(3):
        left_real = left[0][:, inner:inner + 1]
        left_imag = left[1][:, inner:inner + 1]
        right_real = right[0][inner:inner + 1]
        right_imag = right[1][inner:inner + 1]
        real_part = real_part + (left_real * right_real - left_imag * right_imag)
        imag_part = imag_part + (left_real * right_imag + left_imag * right_real)
    return jnp.stack([real_part, imag_part])


def adjoint(matrix):
    return jnp.stack([jnp.swapaxes(matrix[0], 0, 1), -jnp.swapaxes(matrix[1], 0, 1)])


def traceless_part(matrix):
    identity = jnp.eye(3, dtype=jnp.float32)[:, :, None, None, None]
    real_part = 0.5 * (matrix[0] - jnp.swapaxes(matrix[0], 0, 1))
    imag_part = 0.5 * (matrix[1] + jnp.swapaxes(matrix[1], 0, 1))
    trace_imag = (matrix[1][0, 0] + matrix[1][1, 1] + matrix[1][2, 2]) / 3.0
    return jnp.stack([real_part, imag_part - trace_imag * identity])


def complex_times(first, second):
    return (first[0] * second[0] - first[1] * second[1], first[0] * second[1] + first[1] * second[0])


def cayley(matrix):
    identity = jnp.eye(3, dtype=jnp.float32)[:, :, None, None, None]
    numerator = jnp.stack([identity + 0.5 * matrix[0], 0.5 * matrix[1]])
    denominator = jnp.stack([identity - 0.5 * matrix[0], -0.5 * matrix[1]])

    def element(row_index, column):
        return (denominator[0, row_index % 3, column % 3], denominator[1, row_index % 3, column % 3])

    cofactor = []
    for row_index in range(3):
        line = []
        for column in range(3):
            first = complex_times(element(column + 1, row_index + 1), element(column + 2, row_index + 2))
            second = complex_times(element(column + 1, row_index + 2), element(column + 2, row_index + 1))
            line.append((first[0] - second[0], first[1] - second[1]))
        cofactor.append(line)
    determinant = complex_times(element(0, 0), cofactor[0][0])
    for middle in (1, 2):
        extra = complex_times(element(0, middle), cofactor[middle][0])
        determinant = (determinant[0] + extra[0], determinant[1] + extra[1])
    norm_square = determinant[0] * determinant[0] + determinant[1] * determinant[1]
    inverse_det = (determinant[0] / norm_square, -determinant[1] / norm_square)
    real_rows = []
    imag_rows = []
    for row_index in range(3):
        values = [complex_times(cofactor[row_index][column], inverse_det) for column in range(3)]
        real_rows.append(jnp.stack([value[0] for value in values]))
        imag_rows.append(jnp.stack([value[1] for value in values]))
    inverse = jnp.stack([jnp.stack(real_rows), jnp.stack(imag_rows)])
    return matrix_product(numerator, inverse)


def roll_time(matrix, steps):
    shape = matrix.shape
    folded = matrix.reshape(shape[:-1] + (shape[-1] // LT, LT))
    return jnp.roll(folded, -steps, axis=-1).reshape(shape)


def displaced(matrix, direction, steps):
    if direction == 0:
        return jnp.roll(matrix, -steps, axis=-3)
    if direction == 1:
        return jnp.roll(matrix, -steps, axis=-2)
    if direction == 2:
        return jnp.roll(matrix, -steps * LT, axis=-1)
    return roll_time(matrix, steps)


def staple_sums(link_list):
    result = []
    for along in range(4):
        staple = None
        for across in range(4):
            if across == along:
                continue
            ahead_across = displaced(link_list[across], along, 1)
            upper_staple = matrix_product(matrix_product(ahead_across, adjoint(displaced(link_list[along], across, 1))), adjoint(link_list[across]))
            lower_staple = matrix_product(matrix_product(adjoint(ahead_across), adjoint(link_list[along])), link_list[across])
            term = upper_staple + displaced(lower_staple, across, -1)
            staple = term if staple is None else staple + term
        result.append(staple)
    return result


def reference(gauge_links, momenta):
    link_list = [gauge_links[index] for index in range(4)]
    first_staples = staple_sums(link_list)
    half_momenta = []
    new_list = []
    for along in range(4):
        gauge_force = traceless_part(matrix_product(link_list[along], first_staples[along]))
        half_step = momenta[along] - kick_size * gauge_force
        half_momenta.append(half_step)
        new_list.append(matrix_product(cayley(step_size * traceless_part(half_step)), link_list[along]))
    second_staples = staple_sums(new_list)
    final_momenta = []
    trace_total = jnp.float32(0.0)
    for along in range(4):
        loop_matrix = matrix_product(new_list[along], second_staples[along])
        final_momenta.append(half_momenta[along] - kick_size * traceless_part(loop_matrix))
        trace_total = trace_total + jnp.sum(loop_matrix[0][0, 0] + loop_matrix[0][1, 1] + loop_matrix[0][2, 2])
    plaquette = trace_total / (72.0 * NX * NY * NZ * LT)
    return (jnp.stack(new_list), jnp.stack(final_momenta), plaquette)
```

```python
import jax
import jax.numpy as jnp
from jax import lax
from jax.experimental import pallas as pl
from jax.experimental.pallas import tpu as pltpu
from jax.sharding import PartitionSpec as P

LT = 64
kick_size = 0.25
step_size = 0.2
OFF = ((0, 1), (0, 2), (1, 2))
PAIRS = tuple((m, n) for m in range(4) for n in range(m + 1, 4))
F32 = jnp.float32


def others(d):
    return tuple(m for m in range(4) if m != d)


def slot(d, m):
    return others(d).index(m)


def dagger(a):
    return [[(a[j][i][0], -a[j][i][1]) for j in range(3)] for i in range(3)]


def entry(a, b, i, j, ah, bh, want_re=True, want_im=True):
    re = im = None
    for k in range(3):
        ar, ai = a[k][i] if ah else a[i][k]
        br, bi = b[j][k] if bh else b[k][j]
        if want_re:
            t1, t2 = ar * br, ai * bi
            t = t1 + t2 if ah != bh else t1 - t2
            re = t if re is None else re + t
        if want_im:
            u1, u2 = ar * bi, ai * br
            if not ah and not bh:
                u = u1 + u2
            elif ah and not bh:
                u = u1 - u2
            elif bh and not ah:
                u = u2 - u1
            else:
                u = -(u1 + u2)
            im = u if im is None else im + u
    return (re, im)


def product(a, b, ah=False, bh=False):
    return [[entry(a, b, i, j, ah, bh) for j in range(3)] for i in range(3)]


def traceless(a):
    out = []
    for i, j in OFF:
        out.append(0.5 * (a[i][j][0] - a[j][i][0]))
        out.append(0.5 * (a[i][j][1] + a[j][i][1]))
    third = (a[0][0][1] + a[1][1][1] + a[2][2][1]) * (1.0 / 3.0)
    out.append(a[0][0][1] - third)
    out.append(a[1][1][1] - third)
    return out


def cayley(h):
    half = 0.5 * step_size
    x = [half * v for v in h]
    r01, i01, r02, i02, r12, i12, d0, d1 = x
    d2 = -(d0 + d1)
    n01 = r01 * r01 + i01 * i01
    n02 = r02 * r02 + i02 * i02
    n12 = r12 * r12 + i12 * i12
    s0 = -(d0 * d0 + n01 + n02)
    s1 = -(d1 * d1 + n01 + n12)
    s2 = -(d2 * d2 + n02 + n12)
    q = -0.5 * (s0 + s1 + s2)
    a01r = -(d0 + d1) * i01 - (r02 * r12 + i02 * i12)
    a01i = (d0 + d1) * r01 - (i02 * r12 - r02 * i12)
    a02r = -(d0 + d2) * i02 + (r01 * r12 - i01 * i12)
    a02i = (d0 + d2) * r02 + (r01 * i12 + i01 * r12)
    a12r = -(d1 + d2) * i12 - (r01 * r02 + i01 * i02)
    a12i = (d1 + d2) * r12 - (r01 * i02 - i01 * r02)
    delta = (
        -d0 * d1 * d2
        + d0 * n12
        + d1 * n02
        + d2 * n01
        + 2.0 * ((r01 * r12 - i01 * i12) * i02 - (r01 * i12 + i01 * r12) * r02)
    )
    w = 1.0 + q
    inv = 1.0 / (w * w + delta * delta)
    fr, fi = w * inv, delta * inv

    def scaled(re, im):
        return (re * fr - im * fi, re * fi + im * fr)

    m = [[None] * 3 for _ in range(3)]
    for (i, j), (hr, hi), (xr, xi) in (
        ((0, 1), (a01r, a01i), (r01, i01)),
        ((0, 2), (a02r, a02i), (r02, i02)),
        ((1, 2), (a12r, a12i), (r12, i12)),
    ):
        m[i][j] = scaled(2.0 * (hr + xr), 2.0 * (hi + xi))
        m[j][i] = scaled(2.0 * (hr - xr), 2.0 * (xi - hi))
    for i, s, d in ((0, s0, d0), (1, s1, d1), (2, s2, d2)):
        m[i][i] = scaled(2.0 * s + w, 2.0 * d + delta)
    return m


def lane_of():
    return lax.broadcasted_iota(jnp.int32, (8, 128), 1)


def row_of():
    return lax.broadcasted_iota(jnp.int32, (8, 128), 0)


def load_link(ref, m, x):
    return [[(ref[m, 0, i, j, x], ref[m, 1, i, j, x]) for j in range(3)] for i in range(3)]


def comp(ri, i, j):
    return ri * 9 + i * 3 + j


class Ahead:
    def __init__(self, ref, xh, yh, zh):
        self.ref, self.xh, self.yh, self.zh = ref, xh, yh, zh
        self.lane, self.row = lane_of(), row_of()

    def one(self, n, d, x, ri, i, j):
        c = comp(ri, i, j)
        k = slot(d, n)
        if d == 0:
            return self.ref[n, ri, i, j, 1] if x == 0 else self.xh[k * 18 + c]
        v = self.ref[n, ri, i, j, x]
        if d == 1:
            halo = jnp.broadcast_to(self.yh[c, pl.ds(2 * k + x, 1), :], (8, 128))
            return jnp.where(self.row == 7, halo, pltpu.roll(v, 7, 0))
        if d == 2:
            h = self.zh[k * 18 + c]
            if x == 0:
                return pltpu.roll(jnp.where(self.lane < LT, h, v), LT, 1)
            return jnp.where(self.lane < LT, pltpu.roll(v, LT, 1), h)
        return jnp.where((self.lane & (LT - 1)) == LT - 1, pltpu.roll(v, LT - 1, 1), pltpu.roll(v, 127, 1))

    def __call__(self, n, d, x):
        return [[(self.one(n, d, x, 0, i, j), self.one(n, d, x, 1, i, j)) for j in range(3)] for i in range(3)]


def pack_z(a, b):
    return jnp.where(lane_of() < LT, a, pltpu.roll(b, LT, 1))


def pack_kernel(v, xs, ys, zs):
    for n in range(4):
        for ri in range(2):
            for i in range(3):
                for j in range(3):
                    c = comp(ri, i, j)
                    if n != 0:
                        xs[slot(0, n) * 18 + c] = v[n, ri, i, j, 0]
                    if n != 1:
                        k = slot(1, n)
                        for x in range(2):
                            ys[c, pl.ds(2 * k + x, 1), :] = v[n, ri, i, j, x, 0:1, :]
                    if n != 2:
                        zs[slot(2, n) * 18 + c] = pack_z(v[n, ri, i, j, 0], v[n, ri, i, j, 1])
    for c in range(18):
        ys[c, 6:8, :] = jnp.zeros((2, 128), F32)


class Force:
    def __init__(self, f, xs, ys, zs):
        self.f, self.xs, self.ys, self.zs = f, xs, ys, zs
        self.lane, self.row = lane_of(), row_of()
        self.seen = set()

    def put(self, m, c, x, w, minus):
        if (m, c, x) in self.seen:
            self.f[m, c, x] = self.f[m, c, x] - w if minus else self.f[m, c, x] + w
        else:
            self.seen.add((m, c, x))
            self.f[m, c, x] = -w if minus else w

    def here(self, m, x, t, minus):
        for c in range(8):
            self.put(m, c, x, t[c], minus)

    def ahead(self, m, d, x, t, minus):
        k = slot(d, m) if d < 3 else None
        for c in range(8):
            w = t[c]
            if d == 0:
                if x == 0:
                    self.put(m, c, 1, w, minus)
                else:
                    self.xs[k * 8 + c] = -w if minus else w
            elif d == 1:
                self.ys[c, pl.ds(2 * k + x, 1), :] = (-w if minus else w)[7:8, :]
                self.put(m, c, x, jnp.where(self.row == 0, 0.0, pltpu.roll(w, 1, 0)), minus)
            elif d == 2:
                r = pltpu.roll(w, LT, 1)
                self.put(m, c, x, jnp.where(self.lane < LT, 0.0, r), minus)
                if x == 0:
                    self.zs[k * 8 + c] = -r if minus else r
                else:
                    self.zs[k * 8 + c] = jnp.where(self.lane < LT, self.zs[k * 8 + c], -w if minus else w)
            else:
                r = jnp.where((self.lane & (LT - 1)) == 0, pltpu.roll(w, LT + 1, 1), pltpu.roll(w, 1, 1))
                self.put(m, c, x, r, minus)


def corner(ahead, m, n, x):
    return product(ahead(n, m, x), ahead(m, n, x), bh=True)


def add_forces(force, links, c_of):
    for m, n in PAIRS:
        for x in range(2):
            c = c_of(m, n, x)
            vm, vn = load_link(links, m, x), load_link(links, n, x)
            a = product(vn, vm, ah=True)
            force.ahead(m, n, x, traceless(product(a, c)), True)
            force.ahead(n, m, x, traceless(product(c, a)), False)
            t = traceless(product(product(vm, c), vn, bh=True))
            force.here(m, x, t, False)
            force.here(n, x, t, True)


def clear_rows(ys):
    for c in range(8):
        ys[c, 6:8, :] = jnp.zeros((2, 128), F32)


def force_kernel(v, xh, yh, zh, f, xs, ys, zs):
    clear_rows(ys)
    ahead = Ahead(v, xh, yh, zh)
    add_forces(Force(f, xs, ys, zs), v, lambda m, n, x: corner(ahead, m, n, x))


def arrived(xr, yr, zr, m, c, x):
    total = None
    if m != 0 and x == 0:
        total = xr[slot(0, m) * 8 + c]
    if m != 1:
        w = jnp.broadcast_to(yr[c, pl.ds(2 * slot(1, m) + x, 1), :], (8, 128))
        w = jnp.where(row_of() == 0, w, 0.0)
        total = w if total is None else total + w
    if m != 2:
        w = zr[slot(2, m) * 8 + c]
        if x == 1:
            w = pltpu.roll(w, LT, 1)
        w = jnp.where(lane_of() < LT, w, 0.0)
        total = w if total is None else total + w
    return total


def momentum_part(ref, m, c, x):
    if c < 6:
        i, j = OFF[c // 2]
        return ref[m, c % 2, i, j, x]
    return ref[m, 1, c - 6, c - 6, x]


def half_kernel(p, f, xr, yr, zr, h, xs, ys, zs):
    for c in range(8):
        ys[c, 6:8, :] = jnp.zeros((2, 128), F32)
        for m in range(4):
            v = []
            for x in range(2):
                g = f[m, c, x] + arrived(xr, yr, zr, m, c, x)
                v.append(momentum_part(p, m, c, x) - kick_size * g)
                h[m, c, x] = v[x]
                if m != 1:
                    ys[c, pl.ds(2 * slot(1, m) + x, 1), :] = v[x][0:1, :]
            if m != 0:
                xs[slot(0, m) * 8 + c] = v[0]
            if m != 2:
                zs[slot(2, m) * 8 + c] = pack_z(v[0], v[1])


def link_kernel(v, h, out):
    for m in range(4):
        for x in range(2):
            new = product(cayley([h[m, c, x] for c in range(8)]), load_link(v, m, x))
            for i in range(3):
                for j in range(3):
                    out[m, 0, i, j, x] = new[i][j][0]
                    out[m, 1, i, j, x] = new[i][j][1]


def corner_kernel(v, xh, yh, zh, xm, ym, zm, corners, trace, nx, ny, nz):
    def from_halo(ref, base):
        return [[(ref[base + comp(0, i, j)], ref[base + comp(1, i, j)]) for j in range(3)] for i in range(3)]

    for old, mom, new in ((xh, xm, nx), (zh, zm, nz)):
        for k in range(3):
            r = product(cayley([mom[k * 8 + c] for c in range(8)]), from_halo(old, k * 18))
            for i in range(3):
                for j in range(3):
                    new[k * 18 + comp(0, i, j)] = r[i][j][0]
                    new[k * 18 + comp(1, i, j)] = r[i][j][1]
    r = product(cayley([ym[c] for c in range(8)]), from_halo(yh, 0))
    for i in range(3):
        for j in range(3):
            ny[comp(0, i, j)] = r[i][j][0]
            ny[comp(1, i, j)] = r[i][j][1]
    ahead = Ahead(v, nx, ny, nz)
    total = None
    for p, (m, n) in enumerate(PAIRS):
        for x in range(2):
            c = corner(ahead, m, n, x)
            for i in range(3):
                for j in range(3):
                    corners[p, 0, i, j, x] = c[i][j][0]
                    corners[p, 1, i, j, x] = c[i][j][1]
            a = product(load_link(v, n, x), load_link(v, m, x), ah=True)
            for i in range(3):
                t = entry(c, a, i, i, False, False, want_im=False)[0]
                total = t if total is None else total + t
    trace[...] = jnp.broadcast_to(jnp.sum(total, axis=0, keepdims=True), trace.shape)


def second_kernel(v, corners, f, xs, ys, zs, out):
    out[...] = v[...]
    clear_rows(ys)

    def c_of(m, n, x):
        p = PAIRS.index((m, n))
        return [[(corners[p, 0, i, j, x], corners[p, 1, i, j, x]) for j in range(3)] for i in range(3)]

    add_forces(Force(f, xs, ys, zs), v, c_of)


def last_kernel(h, f, xr, yr, zr, traces, out, plaquette):
    total = jnp.sum(traces[...], axis=0, keepdims=True)
    plaquette[...] = jnp.sum(total, axis=1, keepdims=True) * (4.0 / (72.0 * 2 * 8 * 128 * traces.shape[0]))
    for m in range(4):
        for x in range(2):
            u = [h[m, c, x] - kick_size * (f[m, c, x] + arrived(xr, yr, zr, m, c, x)) for c in range(8)]
            for k, (i, j) in enumerate(OFF):
                out[m, 0, i, j, x] = u[2 * k]
                out[m, 0, j, i, x] = -u[2 * k]
                out[m, 1, i, j, x] = u[2 * k + 1]
                out[m, 1, j, i, x] = u[2 * k + 1]
            for i, d in enumerate((u[6], u[7], -(u[6] + u[7]))):
                out[m, 0, i, i, x] = jnp.zeros((8, 128), F32)
                out[m, 1, i, i, x] = d


def call(kernel, shapes, flops, scratch=()):
    def run(*args):
        vmem = pl.BlockSpec(memory_space=pltpu.VMEM)
        return pl.pallas_call(
            kernel,
            out_shape=[jax.ShapeDtypeStruct(s, F32) for s in shapes],
            in_specs=[vmem] * len(args),
            out_specs=[vmem] * len(shapes),
            scratch_shapes=[pltpu.VMEM(s, F32) for s in scratch],
            cost_estimate=pl.CostEstimate(flops=flops, bytes_accessed=2_000_000, transcendentals=0),
            compiler_params=pltpu.CompilerParams(vmem_limit_bytes=VMEM_LIMIT),
            name=kernel.__name__,
        )(*args)

    return run


LINK = (4, 2, 3, 3, 2, 8, 128)
HALO_LINK = ((54, 8, 128), (18, 8, 128), (54, 8, 128))
HALO_MOM = ((24, 8, 128), (8, 8, 128), (24, 8, 128))
MOM = (4, 8, 2, 8, 128)
CORNER = (6, 2, 3, 3, 2, 8, 128)
BIG = 400_000_000
VMEM_LIMIT = 16 * 1024 * 1024


def solution(mesh):
    size = dict(mesh.shape)

    def shift(a, axis, step):
        n = size[axis]
        return lax.ppermute(a, axis, [(i, (i + step) % n) for i in range(n)])

    def halos(arrays, step):
        return [shift(a, axis, step) for a, axis in zip(arrays, ("gx", "gy", "zt"), strict=True)]

    def body(v, p):
        halo = halos(call(pack_kernel, HALO_LINK, 1_000_000)(v), -1)
        f, *up = call(force_kernel, (MOM, *HALO_MOM), BIG)(v, *halo)
        h, *down = call(half_kernel, (MOM, *HALO_MOM), 1_000_000)(p, f, *halos(up, 1))
        down = halos(down, -1)
        (new,) = call(link_kernel, (LINK,), 100_000_000)(v, h)
        corners, trace = call(corner_kernel, (CORNER, (mesh.size, 128)), 100_000_000, HALO_LINK)(new, *halo, *down)
        f, *up, new = call(second_kernel, (MOM, *HALO_MOM, LINK), BIG)(new, corners)
        up, trace = lax.optimization_barrier((up, trace))
        up = halos(up, 1)
        traces = lax.all_to_all(trace, mesh.axis_names, split_axis=0, concat_axis=0, tiled=True)
        last, plaquette = call(last_kernel, (LINK, (1, 1)), 1_000_000)(h, f, *up, traces)
        return new, last, plaquette.reshape(())

    spec = P(None, None, None, None, "gx", "gy", "zt")
    return jax.shard_map(body, mesh=mesh, in_specs=(spec, spec), out_specs=(spec, spec, P()), check_vma=False)
```

```python
import jax
import jax.numpy as jnp
from jax import lax
from jax.experimental import pallas as pl
from jax.experimental.pallas import tpu as pltpu
from jax.sharding import PartitionSpec as P


LT = 64
kick_size = 0.25
step_size = 0.2
OFF = ((0, 1), (0, 2), (1, 2))
PAIRS = tuple((m, n) for m in range(4) for n in range(m + 1, 4))
F32 = jnp.float32


def others(d):
    return tuple(m for m in range(4) if m != d)


def slot(d, m):
    return others(d).index(m)


def entry(a, b, i, j, ah, bh, want_re=True, want_im=True):
    re = im = None
    for k in range(3):
        ar, ai = a[k][i] if ah else a[i][k]
        br, bi = b[j][k] if bh else b[k][j]
        if want_re:
            t1, t2 = ar * br, ai * bi
            t = t1 + t2 if ah != bh else t1 - t2
            re = t if re is None else re + t
        if want_im:
            u1, u2 = ar * bi, ai * br
            if not ah and not bh:
                u = u1 + u2
            elif ah and not bh:
                u = u1 - u2
            elif bh and not ah:
                u = u2 - u1
            else:
                u = -(u1 + u2)
            im = u if im is None else im + u
    return (re, im)


def product(a, b, ah=False, bh=False):
    return [[entry(a, b, i, j, ah, bh) for j in range(3)] for i in range(3)]


def traceless(a):
    out = []
    for i, j in OFF:
        out.append(0.5 * (a[i][j][0] - a[j][i][0]))
        out.append(0.5 * (a[i][j][1] + a[j][i][1]))
    third = (a[0][0][1] + a[1][1][1] + a[2][2][1]) * (1.0 / 3.0)
    out.append(a[0][0][1] - third)
    out.append(a[1][1][1] - third)
    return out


def cayley(h):
    half = 0.5 * step_size
    x = [half * v for v in h]
    r01, i01, r02, i02, r12, i12, d0, d1 = x
    d2 = -(d0 + d1)
    n01 = r01 * r01 + i01 * i01
    n02 = r02 * r02 + i02 * i02
    n12 = r12 * r12 + i12 * i12
    s0 = -(d0 * d0 + n01 + n02)
    s1 = -(d1 * d1 + n01 + n12)
    s2 = -(d2 * d2 + n02 + n12)
    q = -0.5 * (s0 + s1 + s2)
    a01r = -(d0 + d1) * i01 - (r02 * r12 + i02 * i12)
    a01i = (d0 + d1) * r01 - (i02 * r12 - r02 * i12)
    a02r = -(d0 + d2) * i02 + (r01 * r12 - i01 * i12)
    a02i = (d0 + d2) * r02 + (r01 * i12 + i01 * r12)
    a12r = -(d1 + d2) * i12 - (r01 * r02 + i01 * i02)
    a12i = (d1 + d2) * r12 - (r01 * i02 - i01 * r02)
    delta = (
        -d0 * d1 * d2
        + d0 * n12
        + d1 * n02
        + d2 * n01
        + 2.0 * ((r01 * r12 - i01 * i12) * i02 - (r01 * i12 + i01 * r12) * r02)
    )
    w = 1.0 + q
    inv = 1.0 / (w * w + delta * delta)
    fr, fi = w * inv, delta * inv

    def scaled(re, im):
        return (re * fr - im * fi, re * fi + im * fr)

    m = [[None] * 3 for _ in range(3)]
    for (i, j), (hr, hi), (xr, xi) in (
        ((0, 1), (a01r, a01i), (r01, i01)),
        ((0, 2), (a02r, a02i), (r02, i02)),
        ((1, 2), (a12r, a12i), (r12, i12)),
    ):
        m[i][j] = scaled(2.0 * (hr + xr), 2.0 * (hi + xi))
        m[j][i] = scaled(2.0 * (hr - xr), 2.0 * (xi - hi))
    for i, s, d in ((0, s0, d0), (1, s1, d1), (2, s2, d2)):
        m[i][i] = scaled(2.0 * s + w, 2.0 * d + delta)
    return m


def lane_of():
    return lax.broadcasted_iota(jnp.int32, (8, 128), 1)


def row_of():
    return lax.broadcasted_iota(jnp.int32, (8, 128), 0)


def load_link(ref, m, x):
    return [[(ref[m, 0, i, j, x], ref[m, 1, i, j, x]) for j in range(3)] for i in range(3)]


def comp(ri, i, j):
    return ri * 9 + i * 3 + j


class Ahead:
    def __init__(self, ref, xh, yh, zh):
        self.ref, self.xh, self.yh, self.zh = ref, xh, yh, zh
        self.lane, self.row = lane_of(), row_of()

    def one(self, n, d, x, ri, i, j):
        c = comp(ri, i, j)
        k = slot(d, n)
        if d == 0:
            return self.ref[n, ri, i, j, 1] if x == 0 else self.xh[k * 18 + c]
        v = self.ref[n, ri, i, j, x]
        if d == 1:
            halo = jnp.broadcast_to(self.yh[c, pl.ds(2 * k + x, 1), :], (8, 128))
            return jnp.where(self.row == 7, halo, pltpu.roll(v, 7, 0))
        if d == 2:
            h = self.zh[k * 18 + c]
            if x == 0:
                return pltpu.roll(jnp.where(self.lane < LT, h, v), LT, 1)
            return jnp.where(self.lane < LT, pltpu.roll(v, LT, 1), h)
        return jnp.where((self.lane & (LT - 1)) == LT - 1, pltpu.roll(v, LT - 1, 1), pltpu.roll(v, 127, 1))

    def __call__(self, n, d, x):
        return [[(self.one(n, d, x, 0, i, j), self.one(n, d, x, 1, i, j)) for j in range(3)] for i in range(3)]


def pack_z(a, b):
    return jnp.where(lane_of() < LT, a, pltpu.roll(b, LT, 1))


def cross(a, k):
    i, j = (k + 1) % 3, (k + 2) % 3
    (pr, pi), (qr, qi) = a[0][i], a[1][j]
    (rr, ri), (sr, si) = a[0][j], a[1][i]
    return (pr * qr - pi * qi - rr * sr + ri * si, pr * qi + pi * qr - rr * si - ri * sr)


def store_short(ref, base, a):
    dr = di = None
    for k in range(3):
        cr, ci = cross(a, k)
        vr, vi = a[2][k]
        tr, ti = vr * cr - vi * ci, vr * ci + vi * cr
        dr, di = (tr, ti) if dr is None else (dr + tr, di + ti)
    for i in range(2):
        for k in range(3):
            ref[base + 2 * (3 * i + k)] = a[i][k][0]
            ref[base + 2 * (3 * i + k) + 1] = a[i][k][1]
    ref[base + 12] = dr
    ref[base + 13] = di


def load_short(ref, base):
    a = [[(ref[base + 2 * (3 * i + k)], ref[base + 2 * (3 * i + k) + 1]) for k in range(3)] for i in range(2)]
    dr, di = ref[base + 12], ref[base + 13]
    last = []
    for k in range(3):
        cr, ci = cross(a, k)
        last.append((dr * cr + di * ci, di * cr - dr * ci))
    return [*a, last]


def store_flat(ref, base, a):
    for i in range(3):
        for j in range(3):
            ref[base + comp(0, i, j)] = a[i][j][0]
            ref[base + comp(1, i, j)] = a[i][j][1]


def load_flat(ref, base):
    return [[(ref[base + comp(0, i, j)], ref[base + comp(1, i, j)]) for j in range(3)] for i in range(3)]


def pack_kernel(v, xs, ys, zs, rows):
    for n in range(4):
        if n != 0:
            store_short(xs, slot(0, n) * 14, load_link(v, n, 0))
        if n != 1:
            k = slot(1, n)
            for ri in range(2):
                for i in range(3):
                    for j in range(3):
                        for x in range(2):
                            rows[comp(ri, i, j), pl.ds(2 * k + x, 1), :] = v[n, ri, i, j, x, 0:1, :]
        if n != 2:
            a, b = load_link(v, n, 0), load_link(v, n, 1)
            z = [[tuple(pack_z(a[i][j][r], b[i][j][r]) for r in range(2)) for j in range(3)] for i in range(3)]
            store_short(zs, slot(2, n) * 14, z)
    for c in range(18):
        rows[c, 6:8, :] = jnp.zeros((2, 128), F32)
    store_short(ys, 0, load_flat(rows, 0))


class Force:
    def __init__(self, f, xs, ys, zs):
        self.f, self.xs, self.ys, self.zs = f, xs, ys, zs
        self.lane, self.row = lane_of(), row_of()
        self.seen = set()

    def put(self, m, c, x, w, minus):
        if (m, c, x) in self.seen:
            self.f[m, c, x] = self.f[m, c, x] - w if minus else self.f[m, c, x] + w
        else:
            self.seen.add((m, c, x))
            self.f[m, c, x] = -w if minus else w

    def ahead(self, m, d, x, t, minus):
        k = slot(d, m) if d < 3 else None
        for c in range(8):
            w = t[c]
            if d == 0:
                if x == 0:
                    self.put(m, c, 1, w, minus)
                else:
                    self.xs[k * 8 + c] = -w if minus else w
            elif d == 1:
                self.ys[c, pl.ds(2 * k + x, 1), :] = (-w if minus else w)[7:8, :]
                self.put(m, c, x, jnp.where(self.row == 0, 0.0, pltpu.roll(w, 1, 0)), minus)
            elif d == 2:
                r = pltpu.roll(w, LT, 1)
                self.put(m, c, x, jnp.where(self.lane < LT, 0.0, r), minus)
                if x == 0:
                    self.zs[k * 8 + c] = -r if minus else r
                else:
                    self.zs[k * 8 + c] = jnp.where(self.lane < LT, self.zs[k * 8 + c], -w if minus else w)
            else:
                r = jnp.where((self.lane & (LT - 1)) == 0, pltpu.roll(w, LT + 1, 1), pltpu.roll(w, 1, 1))
                self.put(m, c, x, r, minus)


def corner(ahead, m, n, x):
    return product(ahead(n, m, x), ahead(m, n, x), bh=True)


def load_pair(ref, m, n, x):
    p = PAIRS.index((m, n))
    return [[(ref[p, 0, i, j, x], ref[p, 1, i, j, x]) for j in range(3)] for i in range(3)]


def store_pair(ref, m, n, x, a):
    p = PAIRS.index((m, n))
    for i in range(3):
        for j in range(3):
            ref[p, 0, i, j, x] = a[i][j][0]
            ref[p, 1, i, j, x] = a[i][j][1]


def local_kernel(v, out):
    for m, n in PAIRS:
        for x in range(2):
            store_pair(out, m, n, x, product(load_link(v, n, x), load_link(v, m, x), ah=True))


def add_shifted(force, a, m, n, x, c):
    force.ahead(m, n, x, traceless(product(a, c)), True)
    force.ahead(n, m, x, traceless(product(c, a)), False)


def add_upper(links, corners, f, out):
    out[...] = f[...]
    for m, n in PAIRS:
        for x in range(2):
            vm, vn = load_link(links, m, x), load_link(links, n, x)
            t = traceless(product(product(vm, load_pair(corners, m, n, x)), vn, bh=True))
            for c in range(8):
                out[m, c, x] = out[m, c, x] + t[c]
                out[n, c, x] = out[n, c, x] - t[c]


def clear_rows(ys):
    for c in range(8):
        ys[c, 6:8, :] = jnp.zeros((2, 128), F32)


def force_kernel(v, a, xh, yh, zh, f, xs, ys, zs, xw, yw, zw, corners):
    clear_rows(ys)
    for short, whole, count in ((xh, xw, 3), (yh, yw, 1), (zh, zw, 3)):
        for k in range(count):
            store_flat(whole, 18 * k, load_short(short, 14 * k))
    ahead = Ahead(v, xw, yw, zw)
    force = Force(f, xs, ys, zs)
    for m, n in PAIRS:
        for x in range(2):
            c = corner(ahead, m, n, x)
            store_pair(corners, m, n, x, c)
            add_shifted(force, load_pair(a, m, n, x), m, n, x, c)


def upper_kernel(v, corners, f, out):
    add_upper(v, corners, f, out)


def arrived(xr, yr, zr, m, c, x):
    total = None
    if m != 0 and x == 0:
        total = xr[slot(0, m) * 8 + c]
    if m != 1:
        w = jnp.broadcast_to(yr[c, pl.ds(2 * slot(1, m) + x, 1), :], (8, 128))
        w = jnp.where(row_of() == 0, w, 0.0)
        total = w if total is None else total + w
    if m != 2:
        w = zr[slot(2, m) * 8 + c]
        if x == 1:
            w = pltpu.roll(w, LT, 1)
        w = jnp.where(lane_of() < LT, w, 0.0)
        total = w if total is None else total + w
    return total


def momentum_part(ref, m, c, x):
    if c < 6:
        i, j = OFF[c // 2]
        return ref[m, c % 2, i, j, x]
    return ref[m, 1, c - 6, c - 6, x]


def half_kernel(p, f, xr, yr, zr, h, xs, ys, zs):
    for c in range(8):
        ys[c, 6:8, :] = jnp.zeros((2, 128), F32)
        for m in range(4):
            v = []
            for x in range(2):
                g = f[m, c, x] + arrived(xr, yr, zr, m, c, x)
                v.append(momentum_part(p, m, c, x) - kick_size * g)
                h[m, c, x] = v[x]
                if m != 1:
                    ys[c, pl.ds(2 * slot(1, m) + x, 1), :] = v[x][0:1, :]
            if m != 0:
                xs[slot(0, m) * 8 + c] = v[0]
            if m != 2:
                zs[slot(2, m) * 8 + c] = pack_z(v[0], v[1])


def link_kernel(v, h, out):
    for m in range(4):
        for x in range(2):
            new = product(cayley([h[m, c, x] for c in range(8)]), load_link(v, m, x))
            for i in range(3):
                for j in range(3):
                    out[m, 0, i, j, x] = new[i][j][0]
                    out[m, 1, i, j, x] = new[i][j][1]


def corner_kernel(v, a, xh, yh, zh, xm, ym, zm, corners, trace, nx, ny, nz):
    for old, mom, new, count in ((xh, xm, nx, 3), (yh, ym, ny, 1), (zh, zm, nz, 3)):
        for k in range(count):
            store_flat(new, 18 * k, product(cayley([mom[k * 8 + c] for c in range(8)]), load_flat(old, 18 * k)))
    ahead = Ahead(v, nx, ny, nz)
    total = None
    for m, n in PAIRS:
        for x in range(2):
            c = corner(ahead, m, n, x)
            store_pair(corners, m, n, x, c)
            b = load_pair(a, m, n, x)
            for i in range(3):
                t = entry(c, b, i, i, False, False, want_im=False)[0]
                total = t if total is None else total + t
    trace[...] = jnp.broadcast_to(jnp.sum(total, axis=0, keepdims=True), trace.shape)


def second_kernel(a, corners, f, xs, ys, zs):
    clear_rows(ys)
    force = Force(f, xs, ys, zs)
    for m, n in PAIRS:
        for x in range(2):
            add_shifted(force, load_pair(a, m, n, x), m, n, x, load_pair(corners, m, n, x))


def final_kernel(v, corners, f, out, links):
    links[...] = v[...]
    add_upper(v, corners, f, out)


def last_kernel(h, f, xr, yr, zr, traces, out, plaquette):
    total = jnp.sum(traces[...], axis=0, keepdims=True)
    plaquette[...] = jnp.sum(total, axis=1, keepdims=True) * (4.0 / (72.0 * 2 * 8 * 128 * traces.shape[0]))
    for m in range(4):
        for x in range(2):
            u = [h[m, c, x] - kick_size * (f[m, c, x] + arrived(xr, yr, zr, m, c, x)) for c in range(8)]
            for k, (i, j) in enumerate(OFF):
                out[m, 0, i, j, x] = u[2 * k]
                out[m, 0, j, i, x] = -u[2 * k]
                out[m, 1, i, j, x] = u[2 * k + 1]
                out[m, 1, j, i, x] = u[2 * k + 1]
            for i, d in enumerate((u[6], u[7], -(u[6] + u[7]))):
                out[m, 0, i, i, x] = jnp.zeros((8, 128), F32)
                out[m, 1, i, i, x] = d


def call(kernel, shapes, flops, scratch=()):
    def run(*args):
        vmem = pl.BlockSpec(memory_space=pltpu.VMEM)
        return pl.pallas_call(
            kernel,
            out_shape=[jax.ShapeDtypeStruct(s, F32) for s in shapes],
            in_specs=[vmem] * len(args),
            out_specs=[vmem] * len(shapes),
            scratch_shapes=[pltpu.VMEM(s, F32) for s in scratch],
            cost_estimate=pl.CostEstimate(flops=flops, bytes_accessed=2_000_000, transcendentals=0),
            compiler_params=pltpu.CompilerParams(vmem_limit_bytes=VMEM_LIMIT),
        )(*args)

    return run


LINK = (4, 2, 3, 3, 2, 8, 128)
HALO_LINK = ((54, 8, 128), (18, 8, 128), (54, 8, 128))
HALO_SHORT = ((42, 8, 128), (14, 8, 128), (42, 8, 128))
HALO_MOM = ((24, 8, 128), (8, 8, 128), (24, 8, 128))
MOM = (4, 8, 2, 8, 128)
CORNER = (6, 2, 3, 3, 2, 8, 128)
BIG = 400_000_000
VMEM_LIMIT = 16 * 1024 * 1024


def solution(mesh):
    size = dict(mesh.shape)

    def shift(a, axis, step):
        n = size[axis]
        return lax.ppermute(a, axis, [(i, (i + step) % n) for i in range(n)])

    def halos(arrays, step):
        return [shift(a, axis, step) for a, axis in zip(arrays, ("gx", "gy", "zt"), strict=True)]

    def body(v, p):
        halo = halos(call(pack_kernel, HALO_SHORT, 1_000_000, ((18, 8, 128),))(v), -1)
        (a,) = call(local_kernel, (CORNER,), 100_000_000)(v)
        f, *up = call(force_kernel, (MOM, *HALO_MOM, *HALO_LINK, CORNER), BIG)(v, a, *halo)
        up, halo, corners = up[:3], up[3:6], up[6]
        up = halos(up, 1)
        (f,) = call(upper_kernel, (MOM,), 100_000_000)(v, corners, f)
        h, *down = call(half_kernel, (MOM, *HALO_MOM), 1_000_000)(p, f, *up)
        down = halos(down, -1)
        (new,) = call(link_kernel, (LINK,), 100_000_000)(v, h)
        (a,) = call(local_kernel, (CORNER,), 100_000_000)(new)
        corners, trace = call(corner_kernel, (CORNER, (mesh.size, 128)), 100_000_000, HALO_LINK)(new, a, *halo, *down)
        traces = lax.all_to_all(trace, mesh.axis_names, split_axis=0, concat_axis=0, tiled=True)
        f, *up = call(second_kernel, (MOM, *HALO_MOM), 100_000_000)(a, corners)
        up = halos(up, 1)
        f, new = call(final_kernel, (MOM, LINK), 100_000_000)(new, corners, f)
        last, plaquette = call(last_kernel, (LINK, (1, 1)), 1_000_000)(h, f, *up, traces)
        return new, last, plaquette.reshape(())

    spec = P(None, None, None, None, "gx", "gy", "zt")
    return jax.shard_map(body, mesh=mesh, in_specs=(spec, spec), out_specs=(spec, spec, P()), check_vma=False)
```

```python
import jax
import jax.numpy as jnp
from jax import lax
from jax.experimental import pallas as pl
from jax.experimental.pallas import tpu as pltpu
from jax.sharding import PartitionSpec as P


LT = 64
kick_size = 0.25
step_size = 0.2
OFF = ((0, 1), (0, 2), (1, 2))
PAIRS = tuple((m, n) for m in range(4) for n in range(m + 1, 4))
F32 = jnp.float32


def others(d):
    return tuple(m for m in range(4) if m != d)


def slot(d, m):
    return others(d).index(m)


def entry(a, b, i, j, ah, bh, want_re=True, want_im=True):
    re = im = None
    for k in range(3):
        ar, ai = a[k][i] if ah else a[i][k]
        br, bi = b[j][k] if bh else b[k][j]
        if want_re:
            t1, t2 = ar * br, ai * bi
            t = t1 + t2 if ah != bh else t1 - t2
            re = t if re is None else re + t
        if want_im:
            u1, u2 = ar * bi, ai * br
            if not ah and not bh:
                u = u1 + u2
            elif ah and not bh:
                u = u1 - u2
            elif bh and not ah:
                u = u2 - u1
            else:
                u = -(u1 + u2)
            im = u if im is None else im + u
    return (re, im)


def product(a, b, ah=False, bh=False):
    return [[entry(a, b, i, j, ah, bh) for j in range(3)] for i in range(3)]


def traceless(a):
    out = []
    for i, j in OFF:
        out.append(0.5 * (a[i][j][0] - a[j][i][0]))
        out.append(0.5 * (a[i][j][1] + a[j][i][1]))
    third = (a[0][0][1] + a[1][1][1] + a[2][2][1]) * (1.0 / 3.0)
    out.append(a[0][0][1] - third)
    out.append(a[1][1][1] - third)
    return out


def cayley(h):
    half = 0.5 * step_size
    x = [half * v for v in h]
    r01, i01, r02, i02, r12, i12, d0, d1 = x
    d2 = -(d0 + d1)
    n01 = r01 * r01 + i01 * i01
    n02 = r02 * r02 + i02 * i02
    n12 = r12 * r12 + i12 * i12
    s0 = -(d0 * d0 + n01 + n02)
    s1 = -(d1 * d1 + n01 + n12)
    s2 = -(d2 * d2 + n02 + n12)
    q = -0.5 * (s0 + s1 + s2)
    a01r = -(d0 + d1) * i01 - (r02 * r12 + i02 * i12)
    a01i = (d0 + d1) * r01 - (i02 * r12 - r02 * i12)
    a02r = -(d0 + d2) * i02 + (r01 * r12 - i01 * i12)
    a02i = (d0 + d2) * r02 + (r01 * i12 + i01 * r12)
    a12r = -(d1 + d2) * i12 - (r01 * r02 + i01 * i02)
    a12i = (d1 + d2) * r12 - (r01 * i02 - i01 * r02)
    delta = (
        -d0 * d1 * d2
        + d0 * n12
        + d1 * n02
        + d2 * n01
        + 2.0 * ((r01 * r12 - i01 * i12) * i02 - (r01 * i12 + i01 * r12) * r02)
    )
    w = 1.0 + q
    inv = 1.0 / (w * w + delta * delta)
    fr, fi = w * inv, delta * inv

    def scaled(re, im):
        return (re * fr - im * fi, re * fi + im * fr)

    m = [[None] * 3 for _ in range(3)]
    for (i, j), (hr, hi), (xr, xi) in (
        ((0, 1), (a01r, a01i), (r01, i01)),
        ((0, 2), (a02r, a02i), (r02, i02)),
        ((1, 2), (a12r, a12i), (r12, i12)),
    ):
        m[i][j] = scaled(2.0 * (hr + xr), 2.0 * (hi + xi))
        m[j][i] = scaled(2.0 * (hr - xr), 2.0 * (xi - hi))
    for i, s, d in ((0, s0, d0), (1, s1, d1), (2, s2, d2)):
        m[i][i] = scaled(2.0 * s + w, 2.0 * d + delta)
    return m


def lane_of():
    return lax.broadcasted_iota(jnp.int32, (8, 128), 1)


def row_of():
    return lax.broadcasted_iota(jnp.int32, (8, 128), 0)


def load_link(ref, m, x):
    return [[(ref[m, 0, i, j, x], ref[m, 1, i, j, x]) for j in range(3)] for i in range(3)]


def comp(ri, i, j):
    return ri * 9 + i * 3 + j


class Ahead:
    def __init__(self, ref, xh, yh, zh):
        self.ref, self.xh, self.yh, self.zh = ref, xh, yh, zh
        self.lane, self.row = lane_of(), row_of()

    def one(self, n, d, x, ri, i, j):
        c = comp(ri, i, j)
        k = slot(d, n)
        if d == 0:
            return self.ref[n, ri, i, j, 1] if x == 0 else self.xh[k * 18 + c]
        v = self.ref[n, ri, i, j, x]
        if d == 1:
            halo = jnp.broadcast_to(self.yh[c, pl.ds(2 * k + x, 1), :], (8, 128))
            return jnp.where(self.row == 7, halo, pltpu.roll(v, 7, 0))
        if d == 2:
            h = self.zh[k * 18 + c]
            if x == 0:
                return pltpu.roll(jnp.where(self.lane < LT, h, v), LT, 1)
            return jnp.where(self.lane < LT, pltpu.roll(v, LT, 1), h)
        return jnp.where((self.lane & (LT - 1)) == LT - 1, pltpu.roll(v, LT - 1, 1), pltpu.roll(v, 127, 1))

    def __call__(self, n, d, x):
        return [[(self.one(n, d, x, 0, i, j), self.one(n, d, x, 1, i, j)) for j in range(3)] for i in range(3)]


def pack_z(a, b):
    return jnp.where(lane_of() < LT, a, pltpu.roll(b, LT, 1))


def cross(a, k):
    i, j = (k + 1) % 3, (k + 2) % 3
    (pr, pi), (qr, qi) = a[0][i], a[1][j]
    (rr, ri), (sr, si) = a[0][j], a[1][i]
    return (pr * qr - pi * qi - rr * sr + ri * si, pr * qi + pi * qr - rr * si - ri * sr)


def store_short(ref, base, a):
    dr = di = None
    for k in range(3):
        cr, ci = cross(a, k)
        vr, vi = a[2][k]
        tr, ti = vr * cr - vi * ci, vr * ci + vi * cr
        dr, di = (tr, ti) if dr is None else (dr + tr, di + ti)
    for i in range(2):
        for k in range(3):
            ref[base + 2 * (3 * i + k)] = a[i][k][0]
            ref[base + 2 * (3 * i + k) + 1] = a[i][k][1]
    ref[base + 12] = dr
    ref[base + 13] = di


def load_short(ref, base):
    a = [[(ref[base + 2 * (3 * i + k)], ref[base + 2 * (3 * i + k) + 1]) for k in range(3)] for i in range(2)]
    dr, di = ref[base + 12], ref[base + 13]
    last = []
    for k in range(3):
        cr, ci = cross(a, k)
        last.append((dr * cr + di * ci, di * cr - dr * ci))
    return [*a, last]


def store_flat(ref, base, a):
    for i in range(3):
        for j in range(3):
            ref[base + comp(0, i, j)] = a[i][j][0]
            ref[base + comp(1, i, j)] = a[i][j][1]


def load_flat(ref, base):
    return [[(ref[base + comp(0, i, j)], ref[base + comp(1, i, j)]) for j in range(3)] for i in range(3)]


def pack_kernel(v, xs, ys, zs, rows):
    for n in range(4):
        if n != 0:
            store_short(xs, slot(0, n) * 14, load_link(v, n, 0))
        if n != 1:
            k = slot(1, n)
            for ri in range(2):
                for i in range(3):
                    for j in range(3):
                        for x in range(2):
                            rows[comp(ri, i, j), pl.ds(2 * k + x, 1), :] = v[n, ri, i, j, x, 0:1, :]
        if n != 2:
            a, b = load_link(v, n, 0), load_link(v, n, 1)
            z = [[tuple(pack_z(a[i][j][r], b[i][j][r]) for r in range(2)) for j in range(3)] for i in range(3)]
            store_short(zs, slot(2, n) * 14, z)
    for c in range(18):
        rows[c, 6:8, :] = jnp.zeros((2, 128), F32)
    store_short(ys, 0, load_flat(rows, 0))


class Force:
    def __init__(self, f, xs, ys, zs):
        self.f, self.xs, self.ys, self.zs = f, xs, ys, zs
        self.lane, self.row = lane_of(), row_of()
        self.seen = set()

    def put(self, m, c, x, w, minus):
        if (m, c, x) in self.seen:
            self.f[m, c, x] = self.f[m, c, x] - w if minus else self.f[m, c, x] + w
        else:
            self.seen.add((m, c, x))
            self.f[m, c, x] = -w if minus else w

    def ahead(self, m, d, x, t, minus):
        k = slot(d, m) if d < 3 else None
        for c in range(8):
            w = t[c]
            if d == 0:
                if x == 0:
                    self.put(m, c, 1, w, minus)
                else:
                    self.xs[k * 8 + c] = -w if minus else w
            elif d == 1:
                self.ys[c, pl.ds(2 * k + x, 1), :] = (-w if minus else w)[7:8, :]
                self.put(m, c, x, jnp.where(self.row == 0, 0.0, pltpu.roll(w, 1, 0)), minus)
            elif d == 2:
                r = pltpu.roll(w, LT, 1)
                self.put(m, c, x, jnp.where(self.lane < LT, 0.0, r), minus)
                if x == 0:
                    self.zs[k * 8 + c] = -r if minus else r
                else:
                    self.zs[k * 8 + c] = jnp.where(self.lane < LT, self.zs[k * 8 + c], -w if minus else w)
            else:
                r = jnp.where((self.lane & (LT - 1)) == 0, pltpu.roll(w, LT + 1, 1), pltpu.roll(w, 1, 1))
                self.put(m, c, x, r, minus)


def corner(ahead, m, n, x):
    return product(ahead(n, m, x), ahead(m, n, x), bh=True)


def load_pair(ref, m, n, x):
    p = PAIRS.index((m, n))
    return [[(ref[p, 0, i, j, x], ref[p, 1, i, j, x]) for j in range(3)] for i in range(3)]


def store_pair(ref, m, n, x, a):
    p = PAIRS.index((m, n))
    for i in range(3):
        for j in range(3):
            ref[p, 0, i, j, x] = a[i][j][0]
            ref[p, 1, i, j, x] = a[i][j][1]


def local_kernel(v, out):
    for m, n in PAIRS:
        for x in range(2):
            store_pair(out, m, n, x, product(load_link(v, n, x), load_link(v, m, x), ah=True))


def add_shifted(force, a, m, n, x, c):
    force.ahead(m, n, x, traceless(product(a, c)), True)
    force.ahead(n, m, x, traceless(product(c, a)), False)


def add_upper(links, corners, f, out):
    out[...] = f[...]
    for m, n in PAIRS:
        for x in range(2):
            vm, vn = load_link(links, m, x), load_link(links, n, x)
            t = traceless(product(product(vm, load_pair(corners, m, n, x)), vn, bh=True))
            for c in range(8):
                out[m, c, x] = out[m, c, x] + t[c]
                out[n, c, x] = out[n, c, x] - t[c]


def clear_rows(ys):
    for c in range(8):
        ys[c, 6:8, :] = jnp.zeros((2, 128), F32)


def force_kernel(v, a, xh, yh, zh, f, xs, ys, zs, xw, yw, zw, corners):
    clear_rows(ys)
    for short, whole, count in ((xh, xw, 3), (yh, yw, 1), (zh, zw, 3)):
        for k in range(count):
            store_flat(whole, 18 * k, load_short(short, 14 * k))
    ahead = Ahead(v, xw, yw, zw)
    force = Force(f, xs, ys, zs)
    for m, n in PAIRS:
        for x in range(2):
            c = corner(ahead, m, n, x)
            store_pair(corners, m, n, x, c)
            add_shifted(force, load_pair(a, m, n, x), m, n, x, c)


def upper_kernel(v, corners, f, out):
    add_upper(v, corners, f, out)


def arrived(xr, yr, zr, m, c, x):
    total = None
    if m != 0 and x == 0:
        total = xr[slot(0, m) * 8 + c]
    if m != 1:
        w = jnp.broadcast_to(yr[c, pl.ds(2 * slot(1, m) + x, 1), :], (8, 128))
        w = jnp.where(row_of() == 0, w, 0.0)
        total = w if total is None else total + w
    if m != 2:
        w = zr[slot(2, m) * 8 + c]
        if x == 1:
            w = pltpu.roll(w, LT, 1)
        w = jnp.where(lane_of() < LT, w, 0.0)
        total = w if total is None else total + w
    return total


def momentum_part(ref, m, c, x):
    if c < 6:
        i, j = OFF[c // 2]
        return ref[m, c % 2, i, j, x]
    return ref[m, 1, c - 6, c - 6, x]


def half_kernel(p, f, xr, yr, zr, h, xs, ys, zs):
    for c in range(8):
        ys[c, 6:8, :] = jnp.zeros((2, 128), F32)
        for m in range(4):
            v = []
            for x in range(2):
                g = f[m, c, x] + arrived(xr, yr, zr, m, c, x)
                v.append(momentum_part(p, m, c, x) - kick_size * g)
                h[m, c, x] = v[x]
                if m != 1:
                    ys[c, pl.ds(2 * slot(1, m) + x, 1), :] = v[x][0:1, :]
            if m != 0:
                xs[slot(0, m) * 8 + c] = v[0]
            if m != 2:
                zs[slot(2, m) * 8 + c] = pack_z(v[0], v[1])


def link_kernel(v, h, out):
    for m in range(4):
        for x in range(2):
            new = product(cayley([h[m, c, x] for c in range(8)]), load_link(v, m, x))
            for i in range(3):
                for j in range(3):
                    out[m, 0, i, j, x] = new[i][j][0]
                    out[m, 1, i, j, x] = new[i][j][1]


def corner_kernel(v, a, xh, yh, zh, xm, ym, zm, corners, trace, nx, ny, nz):
    for old, mom, new, count in ((xh, xm, nx, 3), (yh, ym, ny, 1), (zh, zm, nz, 3)):
        for k in range(count):
            store_flat(new, 18 * k, product(cayley([mom[k * 8 + c] for c in range(8)]), load_flat(old, 18 * k)))
    ahead = Ahead(v, nx, ny, nz)
    total = None
    for m, n in PAIRS:
        for x in range(2):
            c = corner(ahead, m, n, x)
            store_pair(corners, m, n, x, c)
            b = load_pair(a, m, n, x)
            for i in range(3):
                t = entry(c, b, i, i, False, False, want_im=False)[0]
                total = t if total is None else total + t
    trace[...] = jnp.broadcast_to(jnp.sum(total, axis=0, keepdims=True), trace.shape)


def second_kernel(a, corners, f, xs, ys, zs):
    clear_rows(ys)
    force = Force(f, xs, ys, zs)
    for m, n in PAIRS:
        for x in range(2):
            add_shifted(force, load_pair(a, m, n, x), m, n, x, load_pair(corners, m, n, x))


def final_kernel(v, corners, f, out, links):
    links[...] = v[...]
    add_upper(v, corners, f, out)


def last_kernel(h, f, xr, yr, zr, traces, out, plaquette):
    total = jnp.sum(traces[...], axis=0, keepdims=True)
    plaquette[...] = jnp.sum(total, axis=1, keepdims=True) * (4.0 / (72.0 * 2 * 8 * 128 * traces.shape[0]))
    for m in range(4):
        for x in range(2):
            u = [h[m, c, x] - kick_size * (f[m, c, x] + arrived(xr, yr, zr, m, c, x)) for c in range(8)]
            for k, (i, j) in enumerate(OFF):
                out[m, 0, i, j, x] = u[2 * k]
                out[m, 0, j, i, x] = -u[2 * k]
                out[m, 1, i, j, x] = u[2 * k + 1]
                out[m, 1, j, i, x] = u[2 * k + 1]
            for i, d in enumerate((u[6], u[7], -(u[6] + u[7]))):
                out[m, 0, i, i, x] = jnp.zeros((8, 128), F32)
                out[m, 1, i, i, x] = d


def call(kernel, shapes, flops, scratch=()):
    def run(*args):
        vmem = pl.BlockSpec(memory_space=pltpu.VMEM)
        return pl.pallas_call(
            kernel,
            out_shape=[jax.ShapeDtypeStruct(s, F32) for s in shapes],
            in_specs=[vmem] * len(args),
            out_specs=[vmem] * len(shapes),
            scratch_shapes=[pltpu.VMEM(s, F32) for s in scratch],
            cost_estimate=pl.CostEstimate(flops=flops, bytes_accessed=2_000_000, transcendentals=0),
            compiler_params=pltpu.CompilerParams(vmem_limit_bytes=VMEM_LIMIT),
        )(*args)

    return run


LINK = (4, 2, 3, 3, 2, 8, 128)
HALO_LINK = ((54, 8, 128), (18, 8, 128), (54, 8, 128))
HALO_SHORT = ((42, 8, 128), (14, 8, 128), (42, 8, 128))
HALO_MOM = ((24, 8, 128), (8, 8, 128), (24, 8, 128))
MOM = (4, 8, 2, 8, 128)
CORNER = (6, 2, 3, 3, 2, 8, 128)
BIG = 400_000_000
AXES = ("gx", "gy", "zt")
VMEM_LIMIT = 16 * 1024 * 1024


def solution(mesh):
    size = dict(mesh.shape)

    def shift(a, axis, step):
        n = size[axis]
        return lax.ppermute(a, axis, [(i, (i + step) % n) for i in range(n)])

    def halos(arrays, step):
        out = []
        for a, axis in zip(arrays, AXES, strict=True):
            out.append(shift(a, axis, step))
        return out

    def body(v, p):
        halo = halos(call(pack_kernel, HALO_SHORT, 1_000_000, ((18, 8, 128),))(v), -1)
        (a,) = call(local_kernel, (CORNER,), 100_000_000)(v)
        f, *up = call(force_kernel, (MOM, *HALO_MOM, *HALO_LINK, CORNER), BIG)(v, a, *halo)
        up, halo, corners = up[:3], up[3:6], up[6]
        up = halos(up, 1)
        (f,) = call(upper_kernel, (MOM,), 100_000_000)(v, corners, f)
        h, *down = call(half_kernel, (MOM, *HALO_MOM), 1_000_000)(p, f, *up)
        down = halos(down, -1)
        (new,) = call(link_kernel, (LINK,), 100_000_000)(v, h)
        (a,) = call(local_kernel, (CORNER,), 100_000_000)(new)
        corners, trace = call(corner_kernel, (CORNER, (mesh.size, 128)), 100_000_000, HALO_LINK)(new, a, *halo, *down)
        traces = lax.all_to_all(trace, mesh.axis_names, split_axis=0, concat_axis=0, tiled=True)
        f, *up = call(second_kernel, (MOM, *HALO_MOM), 100_000_000)(a, corners)
        up = halos(up, 1)
        f, new = call(final_kernel, (MOM, LINK), 100_000_000)(new, corners, f)
        last, plaquette = call(last_kernel, (LINK, (1, 1)), 1_000_000)(h, f, *up, traces)
        return new, last, plaquette.reshape(())

    spec = P(None, None, None, None, "gx", "gy", "zt")
    return jax.shard_map(body, mesh=mesh, in_specs=(spec, spec), out_specs=(spec, spec, P()), check_vma=False)
```

```python
import jax
import jax.numpy as jnp
from jax import lax
from jax.experimental import pallas as pl
from jax.experimental.pallas import tpu as pltpu
from jax.sharding import PartitionSpec as P


LT = 64
kick_size = 0.25
step_size = 0.2
OFF = ((0, 1), (0, 2), (1, 2))
PAIRS = tuple((m, n) for m in range(4) for n in range(m + 1, 4))
F32 = jnp.float32


def others(d):
    return tuple(m for m in range(4) if m != d)


def slot(d, m):
    return others(d).index(m)


def entry(a, b, i, j, ah, bh, want_re=True, want_im=True):
    re = im = None
    for k in range(3):
        ar, ai = a[k][i] if ah else a[i][k]
        br, bi = b[j][k] if bh else b[k][j]
        if want_re:
            t1, t2 = ar * br, ai * bi
            t = t1 + t2 if ah != bh else t1 - t2
            re = t if re is None else re + t
        if want_im:
            u1, u2 = ar * bi, ai * br
            if not ah and not bh:
                u = u1 + u2
            elif ah and not bh:
                u = u1 - u2
            elif bh and not ah:
                u = u2 - u1
            else:
                u = -(u1 + u2)
            im = u if im is None else im + u
    return (re, im)


def product(a, b, ah=False, bh=False):
    return [[entry(a, b, i, j, ah, bh) for j in range(3)] for i in range(3)]


def traceless(a):
    out = []
    for i, j in OFF:
        out.append(0.5 * (a[i][j][0] - a[j][i][0]))
        out.append(0.5 * (a[i][j][1] + a[j][i][1]))
    third = (a[0][0][1] + a[1][1][1] + a[2][2][1]) * (1.0 / 3.0)
    out.append(a[0][0][1] - third)
    out.append(a[1][1][1] - third)
    return out


def cayley(h):
    half = 0.5 * step_size
    x = [half * v for v in h]
    r01, i01, r02, i02, r12, i12, d0, d1 = x
    d2 = -(d0 + d1)
    n01 = r01 * r01 + i01 * i01
    n02 = r02 * r02 + i02 * i02
    n12 = r12 * r12 + i12 * i12
    s0 = -(d0 * d0 + n01 + n02)
    s1 = -(d1 * d1 + n01 + n12)
    s2 = -(d2 * d2 + n02 + n12)
    q = -0.5 * (s0 + s1 + s2)
    a01r = -(d0 + d1) * i01 - (r02 * r12 + i02 * i12)
    a01i = (d0 + d1) * r01 - (i02 * r12 - r02 * i12)
    a02r = -(d0 + d2) * i02 + (r01 * r12 - i01 * i12)
    a02i = (d0 + d2) * r02 + (r01 * i12 + i01 * r12)
    a12r = -(d1 + d2) * i12 - (r01 * r02 + i01 * i02)
    a12i = (d1 + d2) * r12 - (r01 * i02 - i01 * r02)
    delta = (
        -d0 * d1 * d2
        + d0 * n12
        + d1 * n02
        + d2 * n01
        + 2.0 * ((r01 * r12 - i01 * i12) * i02 - (r01 * i12 + i01 * r12) * r02)
    )
    w = 1.0 + q
    inv = 1.0 / (w * w + delta * delta)
    fr, fi = w * inv, delta * inv

    def scaled(re, im):
        return (re * fr - im * fi, re * fi + im * fr)

    m = [[None] * 3 for _ in range(3)]
    for (i, j), (hr, hi), (xr, xi) in (
        ((0, 1), (a01r, a01i), (r01, i01)),
        ((0, 2), (a02r, a02i), (r02, i02)),
        ((1, 2), (a12r, a12i), (r12, i12)),
    ):
        m[i][j] = scaled(2.0 * (hr + xr), 2.0 * (hi + xi))
        m[j][i] = scaled(2.0 * (hr - xr), 2.0 * (xi - hi))
    for i, s, d in ((0, s0, d0), (1, s1, d1), (2, s2, d2)):
        m[i][i] = scaled(2.0 * s + w, 2.0 * d + delta)
    return m


def lane_of():
    return lax.broadcasted_iota(jnp.int32, (8, 128), 1)


def row_of():
    return lax.broadcasted_iota(jnp.int32, (8, 128), 0)


def load_link(ref, m, x):
    return [[(ref[m, 0, i, j, x], ref[m, 1, i, j, x]) for j in range(3)] for i in range(3)]


def comp(ri, i, j):
    return ri * 9 + i * 3 + j


class Ahead:
    def __init__(self, ref, xh, yh, zh):
        self.ref, self.xh, self.yh, self.zh = ref, xh, yh, zh
        self.lane, self.row = lane_of(), row_of()

    def one(self, n, d, x, ri, i, j):
        c = comp(ri, i, j)
        k = slot(d, n)
        if d == 0:
            return self.ref[n, ri, i, j, 1] if x == 0 else self.xh[k * 18 + c]
        v = self.ref[n, ri, i, j, x]
        if d == 1:
            halo = jnp.broadcast_to(self.yh[c, pl.ds(2 * k + x, 1), :], (8, 128))
            return jnp.where(self.row == 7, halo, pltpu.roll(v, 7, 0))
        if d == 2:
            h = self.zh[k * 18 + c]
            if x == 0:
                return pltpu.roll(jnp.where(self.lane < LT, h, v), LT, 1)
            return jnp.where(self.lane < LT, pltpu.roll(v, LT, 1), h)
        return jnp.where((self.lane & (LT - 1)) == LT - 1, pltpu.roll(v, LT - 1, 1), pltpu.roll(v, 127, 1))

    def __call__(self, n, d, x):
        return [[(self.one(n, d, x, 0, i, j), self.one(n, d, x, 1, i, j)) for j in range(3)] for i in range(3)]


def pack_z(a, b):
    return jnp.where(lane_of() < LT, a, pltpu.roll(b, LT, 1))


def cross(a, k):
    i, j = (k + 1) % 3, (k + 2) % 3
    (pr, pi), (qr, qi) = a[0][i], a[1][j]
    (rr, ri), (sr, si) = a[0][j], a[1][i]
    return (pr * qr - pi * qi - rr * sr + ri * si, pr * qi + pi * qr - rr * si - ri * sr)


def store_short(ref, base, a):
    dr = di = None
    for k in range(3):
        cr, ci = cross(a, k)
        vr, vi = a[2][k]
        tr, ti = vr * cr - vi * ci, vr * ci + vi * cr
        dr, di = (tr, ti) if dr is None else (dr + tr, di + ti)
    for i in range(2):
        for k in range(3):
            ref[base + 2 * (3 * i + k)] = a[i][k][0]
            ref[base + 2 * (3 * i + k) + 1] = a[i][k][1]
    ref[base + 12] = dr
    ref[base + 13] = di


def load_short(ref, base):
    a = [[(ref[base + 2 * (3 * i + k)], ref[base + 2 * (3 * i + k) + 1]) for k in range(3)] for i in range(2)]
    dr, di = ref[base + 12], ref[base + 13]
    last = []
    for k in range(3):
        cr, ci = cross(a, k)
        last.append((dr * cr + di * ci, di * cr - dr * ci))
    return [*a, last]


def store_flat(ref, base, a):
    for i in range(3):
        for j in range(3):
            ref[base + comp(0, i, j)] = a[i][j][0]
            ref[base + comp(1, i, j)] = a[i][j][1]


def load_flat(ref, base):
    return [[(ref[base + comp(0, i, j)], ref[base + comp(1, i, j)]) for j in range(3)] for i in range(3)]


def pack_kernel(v, xs, ys, zs, rows):
    for n in range(4):
        if n != 0:
            store_short(xs, slot(0, n) * 14, load_link(v, n, 0))
        if n != 1:
            k = slot(1, n)
            for ri in range(2):
                for i in range(3):
                    for j in range(3):
                        for x in range(2):
                            rows[comp(ri, i, j), pl.ds(2 * k + x, 1), :] = v[n, ri, i, j, x, 0:1, :]
        if n != 2:
            a, b = load_link(v, n, 0), load_link(v, n, 1)
            z = [[tuple(pack_z(a[i][j][r], b[i][j][r]) for r in range(2)) for j in range(3)] for i in range(3)]
            store_short(zs, slot(2, n) * 14, z)
    for c in range(18):
        rows[c, 6:8, :] = jnp.zeros((2, 128), F32)
    store_short(ys, 0, load_flat(rows, 0))


class Force:
    def __init__(self, f, xs, ys, zs):
        self.f, self.xs, self.ys, self.zs = f, xs, ys, zs
        self.lane, self.row = lane_of(), row_of()
        self.seen = set()

    def put(self, m, c, x, w, minus):
        if (m, c, x) in self.seen:
            self.f[m, c, x] = self.f[m, c, x] - w if minus else self.f[m, c, x] + w
        else:
            self.seen.add((m, c, x))
            self.f[m, c, x] = -w if minus else w

    def ahead(self, m, d, x, t, minus):
        k = slot(d, m) if d < 3 else None
        for c in range(8):
            w = t[c]
            if d == 0:
                if x == 0:
                    self.put(m, c, 1, w, minus)
                else:
                    self.xs[k * 8 + c] = -w if minus else w
            elif d == 1:
                self.ys[c, pl.ds(2 * k + x, 1), :] = (-w if minus else w)[7:8, :]
                self.put(m, c, x, jnp.where(self.row == 0, 0.0, pltpu.roll(w, 1, 0)), minus)
            elif d == 2:
                r = pltpu.roll(w, LT, 1)
                self.put(m, c, x, jnp.where(self.lane < LT, 0.0, r), minus)
                if x == 0:
                    self.zs[k * 8 + c] = -r if minus else r
                else:
                    self.zs[k * 8 + c] = jnp.where(self.lane < LT, self.zs[k * 8 + c], -w if minus else w)
            else:
                r = jnp.where((self.lane & (LT - 1)) == 0, pltpu.roll(w, LT + 1, 1), pltpu.roll(w, 1, 1))
                self.put(m, c, x, r, minus)


def corner(ahead, m, n, x):
    return product(ahead(n, m, x), ahead(m, n, x), bh=True)


def load_pair(ref, m, n, x):
    p = PAIRS.index((m, n))
    return [[(ref[p, 0, i, j, x], ref[p, 1, i, j, x]) for j in range(3)] for i in range(3)]


def store_pair(ref, m, n, x, a):
    p = PAIRS.index((m, n))
    for i in range(3):
        for j in range(3):
            ref[p, 0, i, j, x] = a[i][j][0]
            ref[p, 1, i, j, x] = a[i][j][1]


def local_kernel(v, out):
    for m, n in PAIRS:
        for x in range(2):
            store_pair(out, m, n, x, product(load_link(v, n, x), load_link(v, m, x), ah=True))


def add_shifted(force, a, m, n, x, c):
    force.ahead(m, n, x, traceless(product(a, c)), True)
    force.ahead(n, m, x, traceless(product(c, a)), False)


def add_upper(links, corners, f, out):
    out[...] = f[...]
    for m, n in PAIRS:
        for x in range(2):
            vm, vn = load_link(links, m, x), load_link(links, n, x)
            t = traceless(product(product(vm, load_pair(corners(m, n), m, n, x)), vn, bh=True))
            for c in range(8):
                out[m, c, x] = out[m, c, x] + t[c]
                out[n, c, x] = out[n, c, x] - t[c]


def clear_rows(ys):
    for c in range(8):
        ys[c, 6:8, :] = jnp.zeros((2, 128), F32)


def early_kernel(v, a, xh, zh, f, xs, zs, xw, zw, corners):
    for short, whole in ((xh, xw), (zh, zw)):
        for k in range(3):
            store_flat(whole, 18 * k, load_short(short, 14 * k))
    ahead = Ahead(v, xw, None, zw)
    force = Force(f, xs, None, zs)
    for m, n in PAIRS:
        if 1 in (m, n):
            continue
        for x in range(2):
            c = corner(ahead, m, n, x)
            store_pair(corners, m, n, x, c)
            add_shifted(force, load_pair(a, m, n, x), m, n, x, c)


def late_kernel(v, a, xw, zw, yh, f1, xs1, zs1, f, xs, ys, zs, yw, corners):
    clear_rows(ys)
    store_flat(yw, 0, load_short(yh, 0))
    force = Force(f, xs, ys, zs)
    for m in others(1):
        f[m] = f1[m]
        force.seen |= {(m, c, x) for c in range(8) for x in range(2)}
        for d, new, old in ((0, xs, xs1), (2, zs, zs1)):
            if m != d:
                new[8 * slot(d, m) : 8 * slot(d, m) + 8] = old[8 * slot(d, m) : 8 * slot(d, m) + 8]
    ahead = Ahead(v, xw, yw, zw)
    for m, n in PAIRS:
        if 1 not in (m, n):
            continue
        for x in range(2):
            c = corner(ahead, m, n, x)
            store_pair(corners, m, n, x, c)
            add_shifted(force, load_pair(a, m, n, x), m, n, x, c)


def upper_kernel(v, early, late, f, out):
    add_upper(v, lambda m, n: late if 1 in (m, n) else early, f, out)


def arrived(xr, yr, zr, m, c, x):
    total = None
    if m != 0 and x == 0:
        total = xr[slot(0, m) * 8 + c]
    if m != 1:
        w = jnp.broadcast_to(yr[c, pl.ds(2 * slot(1, m) + x, 1), :], (8, 128))
        w = jnp.where(row_of() == 0, w, 0.0)
        total = w if total is None else total + w
    if m != 2:
        w = zr[slot(2, m) * 8 + c]
        if x == 1:
            w = pltpu.roll(w, LT, 1)
        w = jnp.where(lane_of() < LT, w, 0.0)
        total = w if total is None else total + w
    return total


def momentum_part(ref, m, c, x):
    if c < 6:
        i, j = OFF[c // 2]
        return ref[m, c % 2, i, j, x]
    return ref[m, 1, c - 6, c - 6, x]


def half_kernel(p, f, xr, yr, zr, h, xs, ys, zs):
    for c in range(8):
        ys[c, 6:8, :] = jnp.zeros((2, 128), F32)
        for m in range(4):
            v = []
            for x in range(2):
                g = f[m, c, x] + arrived(xr, yr, zr, m, c, x)
                v.append(momentum_part(p, m, c, x) - kick_size * g)
                h[m, c, x] = v[x]
                if m != 1:
                    ys[c, pl.ds(2 * slot(1, m) + x, 1), :] = v[x][0:1, :]
            if m != 0:
                xs[slot(0, m) * 8 + c] = v[0]
            if m != 2:
                zs[slot(2, m) * 8 + c] = pack_z(v[0], v[1])


def link_kernel(v, h, out):
    for m in range(4):
        for x in range(2):
            new = product(cayley([h[m, c, x] for c in range(8)]), load_link(v, m, x))
            for i in range(3):
                for j in range(3):
                    out[m, 0, i, j, x] = new[i][j][0]
                    out[m, 1, i, j, x] = new[i][j][1]


def corner_kernel(v, a, xh, yh, zh, xm, ym, zm, corners, trace, nx, ny, nz):
    for old, mom, new, count in ((xh, xm, nx, 3), (yh, ym, ny, 1), (zh, zm, nz, 3)):
        for k in range(count):
            store_flat(new, 18 * k, product(cayley([mom[k * 8 + c] for c in range(8)]), load_flat(old, 18 * k)))
    ahead = Ahead(v, nx, ny, nz)
    total = None
    for m, n in PAIRS:
        for x in range(2):
            c = corner(ahead, m, n, x)
            store_pair(corners, m, n, x, c)
            b = load_pair(a, m, n, x)
            for i in range(3):
                t = entry(c, b, i, i, False, False, want_im=False)[0]
                total = t if total is None else total + t
    trace[...] = jnp.broadcast_to(jnp.sum(total, axis=0, keepdims=True), trace.shape)


def second_kernel(a, corners, f, xs, ys, zs):
    clear_rows(ys)
    force = Force(f, xs, ys, zs)
    for m, n in PAIRS:
        for x in range(2):
            add_shifted(force, load_pair(a, m, n, x), m, n, x, load_pair(corners, m, n, x))


def final_kernel(v, corners, f, out, links):
    links[...] = v[...]
    add_upper(v, lambda m, n: corners, f, out)


def last_kernel(h, f, xr, yr, zr, traces, out, plaquette):
    total = jnp.sum(traces[...], axis=0, keepdims=True)
    plaquette[...] = jnp.sum(total, axis=1, keepdims=True) * (4.0 / (72.0 * 2 * 8 * 128 * traces.shape[0]))
    for m in range(4):
        for x in range(2):
            u = [h[m, c, x] - kick_size * (f[m, c, x] + arrived(xr, yr, zr, m, c, x)) for c in range(8)]
            for k, (i, j) in enumerate(OFF):
                out[m, 0, i, j, x] = u[2 * k]
                out[m, 0, j, i, x] = -u[2 * k]
                out[m, 1, i, j, x] = u[2 * k + 1]
                out[m, 1, j, i, x] = u[2 * k + 1]
            for i, d in enumerate((u[6], u[7], -(u[6] + u[7]))):
                out[m, 0, i, i, x] = jnp.zeros((8, 128), F32)
                out[m, 1, i, i, x] = d


def call(kernel, shapes, flops, scratch=()):
    def run(*args):
        vmem = pl.BlockSpec(memory_space=pltpu.VMEM)
        return pl.pallas_call(
            kernel,
            out_shape=[jax.ShapeDtypeStruct(s, F32) for s in shapes],
            in_specs=[vmem] * len(args),
            out_specs=[vmem] * len(shapes),
            scratch_shapes=[pltpu.VMEM(s, F32) for s in scratch],
            cost_estimate=pl.CostEstimate(flops=flops, bytes_accessed=2_000_000, transcendentals=0),
            compiler_params=pltpu.CompilerParams(vmem_limit_bytes=VMEM_LIMIT),
        )(*args)

    return run


LINK = (4, 2, 3, 3, 2, 8, 128)
HALO_LINK = ((54, 8, 128), (18, 8, 128), (54, 8, 128))
HALO_SHORT = ((42, 8, 128), (14, 8, 128), (42, 8, 128))
HALO_MOM = ((24, 8, 128), (8, 8, 128), (24, 8, 128))
MOM = (4, 8, 2, 8, 128)
CORNER = (6, 2, 3, 3, 2, 8, 128)
AXES = ("gx", "gy", "zt")
VMEM_LIMIT = 16 * 1024 * 1024


def solution(mesh):
    size = dict(mesh.shape)

    def shift(a, axis, step):
        n = size[axis]
        return lax.ppermute(a, axis, [(i, (i + step) % n) for i in range(n)])

    def halos(arrays, step):
        out = []
        for a, axis in zip(arrays, AXES, strict=True):
            out.append(shift(a, axis, step))
        return out

    def body(v, p):
        halo = halos(call(pack_kernel, HALO_SHORT, 1_000_000, ((18, 8, 128),))(v), -1)
        (a,) = call(local_kernel, (CORNER,), 100_000_000)(v)
        xh, yh, zh = halo
        shapes = (MOM, HALO_MOM[0], HALO_MOM[2], HALO_LINK[0], HALO_LINK[2], CORNER)
        f, xs, zs, xh, zh, early = call(early_kernel, shapes, 100_000_000)(v, a, xh, zh)
        shapes = (MOM, *HALO_MOM, HALO_LINK[1], CORNER)
        f, *up, yh, late = call(late_kernel, shapes, 100_000_000)(v, a, xh, zh, yh, f, xs, zs)
        halo = (xh, yh, zh)
        up = halos(up, 1)
        (f,) = call(upper_kernel, (MOM,), 100_000_000)(v, early, late, f)
        h, *down = call(half_kernel, (MOM, *HALO_MOM), 1_000_000)(p, f, *up)
        down = halos(down, -1)
        (new,) = call(link_kernel, (LINK,), 100_000_000)(v, h)
        (a,) = call(local_kernel, (CORNER,), 100_000_000)(new)
        corners, trace = call(corner_kernel, (CORNER, (mesh.size, 128)), 100_000_000, HALO_LINK)(new, a, *halo, *down)
        traces = lax.all_to_all(trace, mesh.axis_names, split_axis=0, concat_axis=0, tiled=True)
        f, *up = call(second_kernel, (MOM, *HALO_MOM), 100_000_000)(a, corners)
        up = halos(up, 1)
        f, new = call(final_kernel, (MOM, LINK), 100_000_000)(new, corners, f)
        last, plaquette = call(last_kernel, (LINK, (1, 1)), 1_000_000)(h, f, *up, traces)
        return new, last, plaquette.reshape(())

    spec = P(None, None, None, None, "gx", "gy", "zt")
    return jax.shard_map(body, mesh=mesh, in_specs=(spec, spec), out_specs=(spec, spec, P()), check_vma=False)
```
